32 devices in a mesh: rows: 8 (over z, y), rep: 4 (over x, core).
Axes of the slice: x: 2, y: 2, z: 4, core: 2. Of those that a mesh axis runs over, the one named last changes fastest.
Arguments:
- tables: bfloat16 [16384, 128], P('rows'), may hold values from -0.5 to 0.5
- indices: int32 [512, 8, 8], P(('rows', 'rep')), may hold values from 0 to 2047
- bag_lengths: int32 [512, 8], P(('rows', 'rep')), may hold values from 1 to 8
- dense: bfloat16 [512, 13], P(('rows', 'rep')), may hold values from -6 to 6
- bottom_first: bfloat16 [13, 512], replicated, may hold values from -1.75 to 1.75
- bottom_second: bfloat16 [512, 256], replicated, may hold values from -0.375 to 0.375
- bottom_third: bfloat16 [256, 128], replicated, may hold values from -0.5 to 0.5
- top_first: bfloat16 [164, 1024], P(None, 'rep'), may hold values from -0.5 to 0.5
- top_second: bfloat16 [1024, 1024], P(None, 'rep'), may hold values from -0.25 to 0.25
- top_third: bfloat16 [1024, 512], P(None, 'rep'), may hold values from -0.25 to 0.25
- top_fourth: bfloat16 [512, 256], P(None, 'rep'), may hold values from -0.375 to 0.375
- top_last: bfloat16 [256], replicated, may hold values from -0.5 to 0.5
Outputs:
- logit: float32 [512], P(('rows', 'rep'))
The draws below stay inside these ranges and needn't reach their ends.
Inputs may be any that keep to these rules, and one draw needn't show every extreme that they name: `indices`: each entry is a row number within its own table; entries at positions of a bag at or past its length are ignored.
All inputs are finite; a program needn't handle non-finite values.
Results may differ from the reference program's by a relative error of at most 0.0076.
Values may be sent and summed in bfloat16 or wider, within the bound.
A program may use at most 64 MiB of HBM per device.

```python
import math
import jax
import jax.numpy as jnp
import numpy as np
from jax import lax

E = 128
DENSE = 13
H1 = 512
H2 = 256
T1 = 1024
T2 = 1024
T3 = 512
T4 = 256
TAB = 8
HOT = 8
TROWS = 2048
NPAIR = 36
BATCH = 512


def place_ends(values, own_key, least, largest):
    longest = values.shape.index(max(values.shape))
    spots = []
    for shift in (0, 1):
        where = [jax.random.randint(jax.random.fold_in(own_key, axis), (), 0, length) for axis, length in enumerate(values.shape)]
        where[longest] = (where[longest] + shift) % values.shape[longest]
        spots.append(tuple(where))
    return values.at[spots[0]].set(least).at[spots[1]].set(largest)


def levels(own_key, dims, split, smallest, top_value):
    def one(position, blocks):
        heights = jax.random.uniform(jax.random.fold_in(jax.random.fold_in(own_key, 6), position), (blocks,), jnp.float32, smallest / len(split), top_value / len(split))
        return jnp.repeat(jnp.exp(heights), dims[position] // blocks).reshape((-1,) + (1,) * (len(dims) - position - 1))

    level = one(*split[0])
    for cut in split[1:]:
        level = level * one(*cut)
    return level


def rank_table(amount, lean):
    weights = [(1 << 20) // math.isqrt(grade ** lean) + 1 for grade in range(1, amount + 1)]
    spread = 1 + sum(weights) // (1 << 30)
    return np.cumsum(np.array([max(1, weight // spread) for weight in weights]))


def skewed_ids(key, extent, number_of, lean):
    table = rank_table(number_of, lean)
    ticket = jax.random.randint(jax.random.fold_in(key, 1), extent, 0, int(table[number_of - 1]))
    grade = jnp.searchsorted(jnp.asarray(table, jnp.int32), ticket, side="right")
    return jax.random.permutation(jax.random.fold_in(key, 2), number_of)[grade].astype(jnp.int32)


def centred(key, dims, deviation, limit, cuts=(), kind=jnp.bfloat16):
    gain = levels(key, dims, cuts, -0.22, 0.18) if cuts else 1.0
    drawn = jax.random.normal(key, dims, jnp.float32) * deviation * gain
    return jnp.minimum(jnp.maximum(drawn, -limit), limit).astype(kind)


def setup_inputs(seed: int = 0) -> dict:
    keys = jax.random.split(jax.random.key(seed), 13)
    return {
        "tables": centred(keys[0], (TAB * TROWS, E), E ** -0.5, 0.5, ((0, 8),)),
        "indices": place_ends(skewed_ids(keys[1], (BATCH, TAB, HOT), TROWS, 2), jax.random.fold_in(keys[1], 3), 0, TROWS - 1).astype(jnp.int32),
        "bag_lengths": place_ends(jax.random.randint(keys[2], (BATCH, TAB), 1, HOT + 1), jax.random.fold_in(keys[2], 1), 1, HOT).astype(jnp.int32),
        "dense": centred(keys[3], (BATCH, DENSE), 1.0, 6.0, ((0, 32),)),
        "bottom_first": centred(keys[4], (DENSE, H1), DENSE ** -0.5, 1.75),
        "bottom_second": centred(keys[5], (H1, H2), (H1 // 2) ** -0.5, 0.375),
        "bottom_third": centred(keys[6], (H2, E), (H2 // 2) ** -0.5, 0.5),
        "top_first": centred(keys[7], (E + NPAIR, T1), (E + NPAIR) ** -0.5, 0.5, ((1, 4),)),
        "top_second": centred(keys[8], (T1, T2), (T1 // 2) ** -0.5, 0.25, ((1, 4),)),
        "top_third": centred(keys[9], (T2, T3), (T2 // 2) ** -0.5, 0.25, ((1, 4),)),
        "top_fourth": centred(keys[10], (T3, T4), (T3 // 2) ** -0.5, 0.375, ((1, 4),)),
        "top_last": centred(keys[11], (T4,), (T4 // 2) ** -0.5, 0.5),
    }


def interact(bottom_out, pooled):
    features = jnp.concatenate([bottom_out[None], pooled], axis=0)
    gram_matrix = jnp.einsum("ibe,jbe->bij", features, features, precision=lax.Precision.HIGHEST)
    left_ids, right_ids = np.triu_indices(TAB + 1, 1)
    pair_dots = gram_matrix[:, left_ids, right_ids]
    return jnp.concatenate([bottom_out, pair_dots], axis=1).astype(jnp.bfloat16)


def bottom_net(dense, bottom_first, bottom_second, bottom_third):
    lower_act = jax.nn.relu(jnp.dot(dense, bottom_first, preferred_element_type=jnp.float32)).astype(jnp.bfloat16)
    middle = jax.nn.relu(jnp.dot(lower_act, bottom_second, preferred_element_type=jnp.float32)).astype(jnp.bfloat16)
    return jax.nn.relu(jnp.dot(middle, bottom_third, preferred_element_type=jnp.float32))


def reference(tables, indices, bag_lengths, dense, bottom_first, bottom_second, bottom_third, top_first, top_second, top_third, top_fourth, top_last):
    def pool_one(carried):
        table_num, table_idx, table_len = carried
        row_ids = (table_num * TROWS + table_idx).astype(jnp.int32)
        live_mask = jnp.arange(HOT, dtype=jnp.int32)[None, :] < table_len[:, None]
        picked = jnp.take(tables, row_ids, axis=0).astype(jnp.float32)
        return jnp.sum(jnp.where(live_mask[:, :, None], picked, jnp.zeros_like(picked)), axis=1)

    pooled = lax.map(pool_one, (jnp.arange(TAB, dtype=jnp.int32), jnp.transpose(indices, (1, 0, 2)), jnp.transpose(bag_lengths)))
    bottom_out = bottom_net(dense, bottom_first, bottom_second, bottom_third)
    activation = interact(bottom_out, pooled)
    for weight_mat in (top_first, top_second, top_third, top_fourth):
        activation = jax.nn.relu(jnp.dot(activation, weight_mat, preferred_element_type=jnp.float32)).astype(jnp.bfloat16)
    return jnp.dot(activation, top_last, preferred_element_type=jnp.float32)
```

```python
import functools

import jax
import jax.numpy as jnp
from jax import lax
from jax.experimental import pallas as pl
from jax.experimental.pallas import tpu as pltpu
from jax.sharding import PartitionSpec as P

TAB = 8
HOT = 8
MESH = pl.DeviceIdType.MESH
BF16 = jnp.bfloat16
F32 = jnp.float32


def flip(k, offset):
    bit = 1
    while bit <= offset:
        if offset & bit:
            k = k + bit - 2 * bit * ((k // bit) % 2)
        bit *= 2
    return k


def dot(a, b):
    return jnp.dot(a, b, preferred_element_type=F32)


def dot_t(a, b):
    return lax.dot_general(a, b, (((1,), (1,)), ((), ())), preferred_element_type=F32)


def relu_round(x):
    return jnp.maximum(x, 0.0).astype(BF16)


def kernel(
    D,
    R,
    tables,
    indices_h,
    lengths_h,
    dense_h,
    bottom_first_h,
    bottom_second_h,
    bottom_third_h,
    top_first,
    top_second,
    top_third,
    top_fourth,
    top_last_h,
    out,
    indices,
    bag_lengths,
    dense,
    bottom_first,
    bottom_second,
    bottom_third,
    top_last,
    table_v,
    w1,
    w2,
    w3,
    w4,
    out_idx,
    recv_idx,
    counts,
    part,
    recv_pool,
    recv_top,
    act1,
    act2,
    recv_act2,
    local_sem,
    e1_send,
    e1_recv,
    e2_send,
    e2_recv,
    e3_send,
    e3_recv,
    e4_send,
    e4_recv,
    w_send,
    w_recv,
):
    B = indices.shape[2]
    rows = tables.shape[0]
    per_table = D // TAB
    me = lax.axis_index("rows")
    k = lax.axis_index("rep")

    barrier = pltpu.get_barrier_semaphore()
    for d in range(1, D):
        pl.semaphore_signal(
            barrier, inc=1, device_id=(lax.rem(me + d, D), k), device_id_type=MESH
        )
    for o in range(1, R):
        pl.semaphore_signal(barrier, inc=1, device_id=(me, flip(k, o)), device_id_type=MESH)

    small = [
        pltpu.make_async_copy(indices_h, indices, local_sem.at[5]),
        pltpu.make_async_copy(lengths_h, bag_lengths, local_sem.at[6]),
        pltpu.make_async_copy(dense_h, dense, local_sem.at[7]),
        pltpu.make_async_copy(bottom_first_h, bottom_first, local_sem.at[8]),
        pltpu.make_async_copy(bottom_second_h, bottom_second, local_sem.at[9]),
        pltpu.make_async_copy(bottom_third_h, bottom_third, local_sem.at[10]),
        pltpu.make_async_copy(top_last_h, top_last, local_sem.at[11]),
    ]
    local = [
        pltpu.make_async_copy(tables, table_v, local_sem.at[0]),
        pltpu.make_async_copy(top_first, w1.at[k], local_sem.at[1]),
        pltpu.make_async_copy(top_second, w2, local_sem.at[2]),
        pltpu.make_async_copy(top_third, w3.at[k], local_sem.at[3]),
        pltpu.make_async_copy(top_fourth, w4.at[k], local_sem.at[4]),
    ]
    for copy in small + local:
        copy.start()

    small[0].wait()
    small[1].wait()
    lens = bag_lengths[...]
    out_idx[...] = jnp.concatenate(
        [jnp.where(lens > s, indices[:, s, :], -1) for s in range(HOT)], axis=1
    ).reshape(TAB, 1, B * HOT)

    pl.semaphore_wait(barrier, D - 1 + R - 1)

    sends = []

    def send(src, dst, ssem, rsem, device):
        copy = pltpu.make_async_remote_copy(
            src_ref=src,
            dst_ref=dst,
            send_sem=ssem,
            recv_sem=rsem,
            device_id=device,
            device_id_type=MESH,
        )
        copy.start()
        sends.append(copy)
        return copy

    first = []
    for d in range(1, D):
        peer = lax.rem(me + d, D)
        first.append(
            send(
                out_idx.at[peer // per_table],
                recv_idx.at[me],
                e1_send.at[d],
                e1_recv.at[d],
                (peer, k),
            )
        )
    recv_idx[me] = out_idx[me // per_table]

    mine = (top_first, top_third, top_fourth)
    whole = (w1, w3, w4)
    arriving = {}
    stages = []
    held = [0]
    bit = R // 2
    while bit:
        stages.append([(bit, h) for h in held])
        held = held + [h ^ bit for h in held]
        bit //= 2

    def weight_send(array, bit, h):
        block = flip(k, h)
        src = mine[array] if h == 0 else whole[array].at[block]
        arriving[array, h ^ bit] = send(
            src,
            whole[array].at[block],
            w_send.at[array * R + (h ^ bit)],
            w_recv.at[array * R + (h ^ bit)],
            (me, flip(k, bit)),
        )

    for array in range(3):
        for stage in stages:
            for bit, h in stage:
                if h == 0:
                    weight_send(array, bit, h)

    got = set()

    def weight_forward(array):
        for stage in stages:
            for bit, h in stage:
                if h != 0:
                    if (array, h) not in got:
                        arriving[array, h].wait_recv()
                        got.add((array, h))
                    weight_send(array, bit, h)

    def weight_finish(array):
        for o in range(1, R):
            if (array, o) not in got:
                arriving[array, o].wait_recv()
                got.add((array, o))

    for copy in small[2:]:
        copy.wait()
    lower = relu_round(dot(dense[...], bottom_first[...]))
    middle = relu_round(dot(lower, bottom_second[...]))
    bottom_out = jnp.maximum(dot(middle, bottom_third[...]), 0.0)

    local[0].wait()
    for copy in first:
        copy.wait_recv()

    offset = (me % per_table) * rows
    cells = lax.broadcasted_iota(jnp.int32, (8, rows), 1)

    def group(g):
        wanted = recv_idx[pl.ds(g * 8, 8)].reshape(8, B * HOT) - offset
        for pair in range(B // 2):
            halves = []
            for b in (2 * pair, 2 * pair + 1):
                total = jnp.zeros((8, rows), F32)
                for s in range(HOT):
                    j = B * s + b
                    total = total + jnp.where(wanted[:, j : j + 1] == cells, 1.0, 0.0)
                halves.append(total)
            counts[16 * pair : 16 * pair + 16, :] = jnp.concatenate(halves, axis=0).astype(BF16)
        partial = dot(counts[...], table_v[...])
        for b in range(B):
            part[pl.ds(g * 8, 8), b, :] = partial[8 * b : 8 * b + 8, :]

    if D == 8:
        group(0)
    else:
        pl.loop(0, D // 8)(group)

    second = []
    for d in range(1, D):
        peer = lax.rem(me + d, D)
        second.append(
            send(part.at[peer], recv_pool.at[me], e2_send.at[d], e2_recv.at[d], (peer, k))
        )
    recv_pool[me] = part[me]
    weight_forward(0)
    for copy in second:
        copy.wait_recv()

    features = [bottom_out]
    for t in range(TAB):
        pooled = recv_pool[t * per_table]
        for i in range(1, per_table):
            pooled = pooled + recv_pool[t * per_table + i]
        features.append(pooled)
    E = bottom_out.shape[1]
    lane = lax.broadcasted_iota(jnp.int32, (B, E), 1)
    dots = jnp.zeros((B, E), F32)
    p = 0
    for i in range(TAB + 1):
        for j in range(i + 1, TAB + 1):
            value = jnp.sum(features[i] * features[j], axis=1, keepdims=True)
            dots = jnp.where(lane == p, value, dots)
            p += 1
    recv_top[k] = jnp.concatenate([bottom_out, dots], axis=1).astype(BF16)

    third = [
        send(recv_top.at[k], recv_top.at[k], e3_send.at[o], e3_recv.at[o], (me, flip(k, o)))
        for o in range(1, R)
    ]
    weight_finish(0)
    weight_forward(1)
    weight_forward(2)
    for copy in local[1:]:
        copy.wait()
    for copy in third:
        copy.wait_recv()

    top_in = recv_top[...].reshape(R * B, 2 * E)
    n1 = w1.shape[2]
    for n in range(R):
        act1[:, n * n1 : (n + 1) * n1] = relu_round(
            dot(top_in[:, :E], w1[n, :E, :]) + dot(top_in[:, E : E + p], w1[n, E:, :])
        )
    act2[...] = relu_round(dot(act1[...], w2[...])).reshape(act2.shape)

    fourth = [
        send(
            act2.at[flip(k, o)], recv_act2.at[k], e4_send.at[o], e4_recv.at[o], (me, flip(k, o))
        )
        for o in range(1, R)
    ]
    recv_act2[k] = act2[k]
    weight_finish(1)
    weight_finish(2)
    for copy in fourth:
        copy.wait_recv()

    third_in = jnp.concatenate([recv_act2[n] for n in range(R)], axis=1)
    fourth_in = jnp.concatenate([relu_round(dot(third_in, w3[n])) for n in range(R)], axis=1)
    last_in = jnp.concatenate([relu_round(dot_t(fourth_in, w4[n])) for n in range(R)], axis=1)
    out[...] = dot_t(top_last[...].reshape(1, -1), last_in).reshape(B)
    for copy in sends:
        copy.wait_send()


def body(*args):
    (tables, indices, bag_lengths, dense, b1, b2, b3, t1, t2, t3, t4, last) = args
    D = lax.axis_size("rows")
    R = lax.axis_size("rep")
    B = indices.shape[0]
    indices = jnp.transpose(indices, (1, 2, 0))
    bag_lengths = jnp.transpose(bag_lengths)
    t4 = jnp.transpose(t4)
    E = tables.shape[1]
    vmem = pl.BlockSpec(memory_space=pltpu.VMEM)
    hbm = pl.BlockSpec(memory_space=pl.ANY)
    dma = pltpu.SemaphoreType.DMA
    result = pl.pallas_call(
        functools.partial(kernel, D, R),
        out_shape=jax.ShapeDtypeStruct((B,), F32),
        in_specs=[hbm] * 12,
        out_specs=vmem,
        scratch_shapes=[
            pltpu.VMEM(indices.shape, jnp.int32),
            pltpu.VMEM(bag_lengths.shape, jnp.int32),
            pltpu.VMEM(dense.shape, BF16),
            pltpu.VMEM(b1.shape, BF16),
            pltpu.VMEM(b2.shape, BF16),
            pltpu.VMEM(b3.shape, BF16),
            pltpu.VMEM(last.shape, BF16),
            pltpu.VMEM(tables.shape, BF16),
            pltpu.VMEM((R,) + t1.shape, BF16),
            pltpu.VMEM(t2.shape, BF16),
            pltpu.VMEM((R,) + t3.shape, BF16),
            pltpu.VMEM((R,) + t4.shape, BF16),
            pltpu.VMEM((TAB, 1, B * HOT), jnp.int32),
            pltpu.VMEM((D, 1, B * HOT), jnp.int32),
            pltpu.VMEM((8 * B, tables.shape[0]), BF16),
            pltpu.VMEM((D, B, E), F32),
            pltpu.VMEM((D, B, E), F32),
            pltpu.VMEM((R, B, 2 * E), BF16),
            pltpu.VMEM((R * B, R * t1.shape[1]), BF16),
            pltpu.VMEM((R, B, t2.shape[1]), BF16),
            pltpu.VMEM((R, B, t2.shape[1]), BF16),
            dma((12,)),
            dma((D,)),
            dma((D,)),
            dma((D,)),
            dma((D,)),
            dma((R,)),
            dma((R,)),
            dma((R,)),
            dma((R,)),
            dma((3 * R,)),
            dma((3 * R,)),
        ],
        compiler_params=pltpu.CompilerParams(collective_id=0, has_side_effects=True),
    )(tables, indices, bag_lengths, dense, b1, b2, b3, t1, t2, t3, t4, last)
    return result


def solution(mesh):
    placed = (
        P("rows", None),
        P(("rows", "rep"), None, None),
        P(("rows", "rep"), None),
        P(("rows", "rep"), None),
        P(),
        P(),
        P(),
        P(None, "rep"),
        P(None, "rep"),
        P(None, "rep"),
        P(None, "rep"),
        P(),
    )
    return jax.shard_map(
        body, mesh=mesh, in_specs=placed, out_specs=P(("rows", "rep")), check_vma=False
    )
```

```python
import functools

import jax
import jax.numpy as jnp
from jax import lax
from jax.experimental import pallas as pl
from jax.experimental.pallas import tpu as pltpu
from jax.sharding import PartitionSpec as P

TAB = 8
HOT = 8
LANES = 128
MESH = pl.DeviceIdType.MESH
BF16 = jnp.bfloat16
F32 = jnp.float32


def flip(k, offset):
    bit = 1
    while bit <= offset:
        if offset & bit:
            k = k + bit - 2 * bit * ((k // bit) % 2)
        bit *= 2
    return k


def dot(a, b):
    return jnp.dot(a, b, preferred_element_type=F32)


def dot_t(a, b):
    return lax.dot_general(a, b, (((1,), (1,)), ((), ())), preferred_element_type=F32)


def run_half(lookup, base, count):
    if count == 4:
        lookup(base)
    else:
        pl.loop(0, count // 4)(lambda g: lookup(base + 4 * g))


def relu_round(x):
    return jnp.maximum(x, 0.0).astype(BF16)


def kernel(
    D,
    R,
    tables,
    indices_h,
    lengths_h,
    dense_h,
    bottom_first_h,
    bottom_second_h,
    bottom_third_h,
    top_first,
    top_second,
    top_third,
    top_fourth,
    top_last_h,
    out,
    indices,
    bag_lengths,
    dense,
    bottom_first,
    bottom_second,
    bottom_third,
    top_last,
    table_v,
    w1,
    w2,
    w3,
    w4,
    out_idx,
    recv_idx,
    counts,
    part,
    recv_pool,
    recv_top,
    act1,
    act2,
    recv_act2,
    local_sem,
    e1_send,
    e1_recv,
    e2_send,
    e2_recv,
    e3_send,
    e3_recv,
    e4_send,
    e4_recv,
    w_send,
    w_recv,
):
    B = indices.shape[2]
    rows = tables.shape[0]
    per_table = D // TAB
    me = lax.axis_index("rows")
    k = lax.axis_index("rep")

    barrier = pltpu.get_barrier_semaphore()
    for d in range(1, D):
        pl.semaphore_signal(
            barrier, inc=1, device_id=(lax.rem(me + d, D), k), device_id_type=MESH
        )
    for o in range(1, R):
        pl.semaphore_signal(barrier, inc=1, device_id=(me, flip(k, o)), device_id_type=MESH)

    small = [
        pltpu.make_async_copy(indices_h, indices, local_sem.at[5]),
        pltpu.make_async_copy(lengths_h, bag_lengths, local_sem.at[6]),
        pltpu.make_async_copy(dense_h, dense, local_sem.at[7]),
        pltpu.make_async_copy(bottom_first_h, bottom_first, local_sem.at[8]),
        pltpu.make_async_copy(bottom_second_h, bottom_second, local_sem.at[9]),
        pltpu.make_async_copy(bottom_third_h, bottom_third, local_sem.at[10]),
        pltpu.make_async_copy(top_last_h, top_last, local_sem.at[11]),
    ]
    local = [
        pltpu.make_async_copy(tables, table_v, local_sem.at[0]),
        pltpu.make_async_copy(top_first, w1.at[k], local_sem.at[1]),
        pltpu.make_async_copy(top_second, w2, local_sem.at[2]),
        pltpu.make_async_copy(top_third, w3.at[k], local_sem.at[3]),
        pltpu.make_async_copy(top_fourth, w4.at[k], local_sem.at[4]),
    ]
    for copy in small + local:
        copy.start()

    small[0].wait()
    small[1].wait()
    lens = bag_lengths[...]
    out_idx[...] = jnp.concatenate(
        [jnp.where(lens > s, indices[:, s, :], -1) for s in range(HOT)], axis=1
    ).reshape(TAB, 1, B * HOT)

    pl.semaphore_wait(barrier, D - 1 + R - 1)

    sends = []

    def send(src, dst, ssem, rsem, device):
        copy = pltpu.make_async_remote_copy(
            src_ref=src,
            dst_ref=dst,
            send_sem=ssem,
            recv_sem=rsem,
            device_id=device,
            device_id_type=MESH,
        )
        copy.start()
        sends.append(copy)
        return copy

    first = {}
    for d in reversed(range(1, D)):
        peer = flip(me, d)
        first[d] = send(
            out_idx.at[peer // per_table], recv_idx.at[me], e1_send.at[d], e1_recv.at[d], (peer, k)
        )
    recv_idx[me] = out_idx[me // per_table]

    mine = (top_first, top_third, top_fourth)
    whole = (w1, w3, w4)
    arriving = {}
    stages = []
    held = [0]
    bit = R // 2
    while bit:
        stages.append([(bit, h) for h in held])
        held = held + [h ^ bit for h in held]
        bit //= 2

    def weight_send(array, bit, h):
        block = flip(k, h)
        src = mine[array] if h == 0 else whole[array].at[block]
        arriving[array, h ^ bit] = send(
            src,
            whole[array].at[block],
            w_send.at[array * R + (h ^ bit)],
            w_recv.at[array * R + (h ^ bit)],
            (me, flip(k, bit)),
        )

    for array in range(3):
        for stage in stages:
            for bit, h in stage:
                if h == 0:
                    weight_send(array, bit, h)

    got = set()

    def weight_forward(array):
        for stage in stages:
            for bit, h in stage:
                if h != 0:
                    if (array, h) not in got:
                        arriving[array, h].wait_recv()
                        got.add((array, h))
                    weight_send(array, bit, h)

    def weight_finish(array):
        for o in range(1, R):
            if (array, o) not in got:
                arriving[array, o].wait_recv()
                got.add((array, o))

    for copy in small[2:]:
        copy.wait()
    lower = relu_round(dot(dense[...], bottom_first[...]))
    middle = relu_round(dot(lower, bottom_second[...]))
    bottom_out = jnp.maximum(dot(middle, bottom_third[...]), 0.0)

    local[0].wait()

    offset = (me % per_table) * rows
    lanes = lax.broadcasted_iota(jnp.int32, (16, LANES), 1).astype(F32).astype(BF16)
    one, zero = jnp.ones((16, LANES), BF16), jnp.zeros((16, LANES), BF16)
    half = B // 2

    def lookup(base):
        rows4 = recv_idx[pl.ds(base, 4)].reshape(4, B * HOT) - offset
        wanted = jnp.concatenate([rows4, pltpu.roll(rows4, B * HOT - half, 1)], axis=0)
        blocks = rows // LANES
        for pair in range(half // 2):
            totals = [jnp.zeros((16, LANES), BF16)] * blocks
            for s in range(HOT):
                j = B * s + 2 * pair
                entry = jnp.concatenate([wanted[:, j : j + 1], wanted[:, j + 1 : j + 2]], axis=0)
                entry = jnp.broadcast_to(entry, (16, LANES))
                high_part = (entry >> 7).astype(F32).astype(BF16)
                low_part = (entry & (LANES - 1)).astype(F32).astype(BF16)
                hit = jnp.where(low_part == lanes, one, zero)
                for n in range(blocks):
                    here = jnp.where(high_part == jnp.asarray(n, BF16), hit, zero)
                    totals[n] = totals[n] + here
            for n in range(blocks):
                counts[16 * pair : 16 * pair + 16, n * LANES : (n + 1) * LANES] = totals[n]
        partial = dot(counts[...], table_v[...])
        for b in range(half):
            part[pl.ds(base, 4), b, :] = partial[8 * b : 8 * b + 4, :]
            part[pl.ds(base, 4), b + half, :] = partial[8 * b + 4 : 8 * b + 8, :]

    second = []

    def second_send(d):
        peer = flip(me, d)
        second.append(
            send(part.at[peer], recv_pool.at[me], e2_send.at[d], e2_recv.at[d], (peer, k))
        )

    low, high = D // 2, D
    for d in range(1, low):
        first[d].wait_recv()
    run_half(lookup, me // low * low, low)
    for d in range(1, low):
        second_send(d)
    for d in range(low, high):
        first[d].wait_recv()
    run_half(lookup, (1 - me // low) * low, low)
    for d in range(low, high):
        second_send(d)
    recv_pool[me] = part[me]
    weight_forward(0)
    for copy in second:
        copy.wait_recv()

    features = [bottom_out]
    for t in range(TAB):
        pooled = recv_pool[t * per_table]
        for i in range(1, per_table):
            pooled = pooled + recv_pool[t * per_table + i]
        features.append(pooled)
    E = bottom_out.shape[1]
    lane = lax.broadcasted_iota(jnp.int32, (B, E), 1)
    dots = jnp.zeros((B, E), F32)
    p = 0
    for i in range(TAB + 1):
        for j in range(i + 1, TAB + 1):
            value = jnp.sum(features[i] * features[j], axis=1, keepdims=True)
            dots = jnp.where(lane == p, value, dots)
            p += 1
    recv_top[k] = jnp.concatenate([bottom_out, dots], axis=1).astype(BF16)

    third = [
        send(recv_top.at[k], recv_top.at[k], e3_send.at[o], e3_recv.at[o], (me, flip(k, o)))
        for o in range(1, R)
    ]
    weight_finish(0)
    weight_forward(1)
    weight_forward(2)
    for copy in local[1:]:
        copy.wait()
    for copy in third:
        copy.wait_recv()

    top_in = recv_top[...].reshape(R * B, 2 * E)
    n1 = w1.shape[2]
    for n in range(R):
        act1[:, n * n1 : (n + 1) * n1] = relu_round(
            dot(top_in[:, :E], w1[n, :E, :]) + dot(top_in[:, E : E + p], w1[n, E:, :])
        )
    act2[...] = relu_round(dot(act1[...], w2[...])).reshape(act2.shape)

    fourth = [
        send(
            act2.at[flip(k, o)], recv_act2.at[k], e4_send.at[o], e4_recv.at[o], (me, flip(k, o))
        )
        for o in range(1, R)
    ]
    recv_act2[k] = act2[k]
    weight_finish(1)
    weight_finish(2)
    for copy in fourth:
        copy.wait_recv()

    third_in = jnp.concatenate([recv_act2[n] for n in range(R)], axis=1)
    fourth_in = jnp.concatenate([relu_round(dot(third_in, w3[n])) for n in range(R)], axis=1)
    last_in = jnp.concatenate([relu_round(dot_t(fourth_in, w4[n])) for n in range(R)], axis=1)
    out[...] = dot_t(top_last[...].reshape(1, -1), last_in).reshape(B)
    for copy in sends:
        copy.wait_send()


def body(*args):
    (tables, indices, bag_lengths, dense, b1, b2, b3, t1, t2, t3, t4, last) = args
    D = lax.axis_size("rows")
    R = lax.axis_size("rep")
    B = indices.shape[0]
    indices = jnp.transpose(indices, (1, 2, 0))
    bag_lengths = jnp.transpose(bag_lengths)
    t4 = jnp.transpose(t4)
    E = tables.shape[1]
    vmem = pl.BlockSpec(memory_space=pltpu.VMEM)
    hbm = pl.BlockSpec(memory_space=pl.ANY)
    dma = pltpu.SemaphoreType.DMA
    result = pl.pallas_call(
        functools.partial(kernel, D, R),
        out_shape=jax.ShapeDtypeStruct((B,), F32),
        in_specs=[hbm] * 12,
        out_specs=vmem,
        scratch_shapes=[
            pltpu.VMEM(indices.shape, jnp.int32),
            pltpu.VMEM(bag_lengths.shape, jnp.int32),
            pltpu.VMEM(dense.shape, BF16),
            pltpu.VMEM(b1.shape, BF16),
            pltpu.VMEM(b2.shape, BF16),
            pltpu.VMEM(b3.shape, BF16),
            pltpu.VMEM(last.shape, BF16),
            pltpu.VMEM(tables.shape, BF16),
            pltpu.VMEM((R,) + t1.shape, BF16),
            pltpu.VMEM(t2.shape, BF16),
            pltpu.VMEM((R,) + t3.shape, BF16),
            pltpu.VMEM((R,) + t4.shape, BF16),
            pltpu.VMEM((TAB, 1, B * HOT), jnp.int32),
            pltpu.VMEM((D, 1, B * HOT), jnp.int32),
            pltpu.VMEM((4 * B, tables.shape[0]), BF16),
            pltpu.VMEM((D, B, E), F32),
            pltpu.VMEM((D, B, E), F32),
            pltpu.VMEM((R, B, 2 * E), BF16),
            pltpu.VMEM((R * B, R * t1.shape[1]), BF16),
            pltpu.VMEM((R, B, t2.shape[1]), BF16),
            pltpu.VMEM((R, B, t2.shape[1]), BF16),
            dma((12,)),
            dma((D,)),
            dma((D,)),
            dma((D,)),
            dma((D,)),
            dma((R,)),
            dma((R,)),
            dma((R,)),
            dma((R,)),
            dma((3 * R,)),
            dma((3 * R,)),
        ],
        compiler_params=pltpu.CompilerParams(collective_id=0, has_side_effects=True),
    )(tables, indices, bag_lengths, dense, b1, b2, b3, t1, t2, t3, t4, last)
    return result


def solution(mesh):
    placed = (
        P("rows", None),
        P(("rows", "rep"), None, None),
        P(("rows", "rep"), None),
        P(("rows", "rep"), None),
        P(),
        P(),
        P(),
        P(None, "rep"),
        P(None, "rep"),
        P(None, "rep"),
        P(None, "rep"),
        P(),
    )
    return jax.shard_map(
        body, mesh=mesh, in_specs=placed, out_specs=P(("rows", "rep")), check_vma=False
    )
```
